256 devices in a mesh: row: 8 (over y, core), col: 32 (over z, x).
Axes of the slice: x: 4, y: 4, z: 8, core: 2. Of those that a mesh axis runs over, the one named last changes fastest.
Arguments:
- residuals: bfloat16 [131072, 32], P(('row', 'col')), may hold values from -6 to 6
- intersect_blocks: int32 [256, 4], P(('row', 'col')), may hold values from 0 to 3
- local_inverse: bfloat16 [131072, 1024], P(('row', 'col')), may hold values from -0.1875 to 0.1875
- coarse_basis: float32 [262144, 64], P(('row', 'col')), may hold values from -0.1875 to 0.1875
- coarse_slots: int32 [16384], replicated, may hold values from 0 to 16383, each once
- coarse_inverse: float32 [16384, 16384], P('row', 'col'), may hold values from -0.1875 to 0.1875
Outputs:
- preconditioned: float32 [131072, 32], P(('row', 'col'))
The draws below stay inside these ranges and needn't reach their ends.
Inputs may be any that keep to these rules, and one draw needn't show every extreme that they name: `intersect_blocks`: each entry names one of the four owned blocks. `coarse_slots`: every coarse index from 0 to 16383 appears exactly once.
All inputs are finite; a program needn't handle non-finite values.
Results may differ from the reference program's by a relative error of at most 0.0003.
Values may be sent and summed in bfloat16 or wider, within the bound.
A program may use at most 64 MiB of HBM per device.

```python
import jax
import jax.numpy as jnp
from jax import lax

BLK = 128
OWN = 512
LOC = 1024
RHS = 32
NEV = 64
COARSE = 16384
DOFS = 131072
N_ROW = 8
N_COL = 32
DEVICES = 256


def set_ends(array, rng, smallest, largest):
    shape = array.shape
    spot = [jax.random.randint(jax.random.fold_in(rng, axis), (), 0, shape[axis]) for axis in range(len(shape))]
    array = array.at[tuple(spot)].set(smallest)
    longest = shape.index(max(shape))
    spot[longest] = (spot[longest] + 1) % shape[longest]
    return array.at[tuple(spot)].set(largest)


def shard_levels(own_key, extent, shards, smallest, high):
    loudness = 1.0
    for position, parts in shards:
        steps = jax.random.uniform(jax.random.fold_in(jax.random.fold_in(own_key, 6), position), (parts,), jnp.float32, smallest / len(shards), high / len(shards))
        loudness = loudness * jnp.repeat(jnp.exp(steps), extent[position] // parts).reshape((-1,) + (1,) * (len(extent) - 1 - position))
    return loudness


def bell_draw(own_key, shape, scale, bound, split=(), kind=jnp.bfloat16):
    array = jax.random.normal(own_key, shape, jnp.float32) * scale
    if len(split) > 0:
        array = shard_levels(own_key, shape, split, -0.22, 0.18) * array
    return jnp.clip(array, min=-bound, max=bound).astype(kind)


def setup_inputs(seed: int = 0) -> dict:
    keys = jax.random.split(jax.random.key(seed), 7)
    return {
        "residuals": bell_draw(keys[0], (DOFS, RHS), 1.0, 6.0, ((0, 256),)),
        "intersect_blocks": set_ends(jax.random.randint(keys[1], (DEVICES, 4), 0, 4), jax.random.fold_in(keys[1], 1), 0, 3).astype(jnp.int32),
        "local_inverse": bell_draw(keys[2], (DOFS, LOC), LOC ** -0.5, 0.1875, ((0, 256),)),
        "coarse_basis": bell_draw(keys[3], (DEVICES * LOC, NEV), LOC ** -0.5, 0.1875, ((0, 256),), jnp.float32),
        "coarse_slots": jax.random.permutation(keys[4], COARSE).astype(jnp.int32),
        "coarse_inverse": bell_draw(keys[5], (COARSE, COARSE), (COARSE // 16) ** -0.5, 0.1875, ((0, 8), (1, 32)), jnp.float32),
    }


def shift_grid(field, axis, by):
    count = field.shape[axis]
    moved = jnp.roll(field, by, axis=axis)
    source = jnp.arange(count, dtype=jnp.int32) - by
    valid = ((source >= 0) & (source < count)).astype(field.dtype)
    shape = [1] * field.ndim
    shape[axis] = count
    return moved * valid.reshape(shape)


def local_product(pair):
    return jnp.dot(pair[0], pair[1], preferred_element_type=jnp.float32)


def reference(residuals, intersect_blocks, local_inverse, coarse_basis, coarse_slots, coarse_inverse):
    nrows = N_ROW
    ncols = N_COL
    blocks = residuals.reshape(nrows, ncols, OWN // BLK, BLK, RHS)
    sends = intersect_blocks.reshape(nrows, ncols, 4).astype(jnp.int32)
    outgoing = jnp.take_along_axis(blocks, sends[:, :, :, None, None], axis=2)
    incoming = jnp.stack([shift_grid(outgoing[:, :, 0], 0, 1), shift_grid(outgoing[:, :, 1], 0, -1),
                          shift_grid(outgoing[:, :, 2], 1, 1), shift_grid(outgoing[:, :, 3], 1, -1)], axis=2)
    local_vec = jnp.concatenate([residuals.reshape(nrows, ncols, OWN, RHS),
                                 incoming.reshape(nrows, ncols, LOC - OWN, RHS)], axis=2).reshape(DEVICES, LOC, RHS)
    inverse = local_inverse.reshape(DEVICES, OWN, LOC)
    schwarz = lax.map(local_product, (inverse, local_vec))
    basis = coarse_basis.reshape(DEVICES, LOC, NEV)
    partial_value = jnp.einsum("dln,dlr->dnr", basis, local_vec.astype(jnp.float32), precision=lax.Precision.HIGHEST)
    coarse_rhs = jnp.zeros((COARSE, RHS), jnp.float32).at[coarse_slots].set(partial_value.reshape(COARSE, RHS))
    coarse_sol = jnp.dot(coarse_inverse, coarse_rhs, precision=lax.Precision.HIGHEST)
    own_coarse = coarse_sol[coarse_slots].reshape(DEVICES, NEV, RHS)
    prolonged = jnp.einsum("dln,dnr->dlr", basis, own_coarse, precision=lax.Precision.HIGHEST)
    grid = prolonged.reshape(nrows, ncols, LOC, RHS)
    returning = grid[:, :, OWN:].reshape(nrows, ncols, 4, BLK, RHS)
    returned = jnp.stack([shift_grid(returning[:, :, 0], 0, -1), shift_grid(returning[:, :, 1], 0, 1),
                          shift_grid(returning[:, :, 2], 1, -1), shift_grid(returning[:, :, 3], 1, 1)], axis=2)
    matches = (sends[..., None] == jnp.arange(OWN // BLK, dtype=jnp.int32)).astype(jnp.float32)
    added = jnp.einsum("rcdb,rcdkq->rcbkq", matches, returned, precision=lax.Precision.HIGHEST)
    result = schwarz.reshape(nrows, ncols, OWN, RHS) + grid[:, :, :OWN] + added.reshape(nrows, ncols, OWN, RHS)
    return result.reshape(DOFS, RHS)
```

```python
import functools

import jax
import jax.numpy as jnp
from jax import lax
from jax.experimental import pallas as pl
from jax.experimental.pallas import tpu as pltpu
from jax.sharding import Mesh
from jax.sharding import PartitionSpec as P

MESH = pl.DeviceIdType.MESH
AXES = ("row_0", "row_1", "col_0", "col_1")
ROW_COL = AXES
ROW = AXES[:2]
COL = AXES[2:]
NY, NK, NZ, NX = 4, 2, 8, 4
NR = NY * NK
BLK = 128
OWN = 512
LOC = 1024
NEV = 64
RHS = 32
LANES = 128
PART = 2048
CHUNKS = 2
WIDTH = PART // CHUNKS
ROWS = WIDTH // LANES
F32 = jnp.float32
BF16 = jnp.bfloat16
NT = (((1,), (1,)), ((), ()))


def dot(a, b):
    return jnp.dot(a, b, preferred_element_type=F32)


def dot_nt(a, b):
    return lax.dot_general(a, b, NT, preferred_element_type=F32)


def halves(x):
    high = x.astype(BF16)
    return high, (x - high.astype(F32)).astype(BF16)


def kernel(
    ib, resid, slots, basis_hbm, linv_hbm, cinv_hbm, out,
    basis, linv, cinv, chigh, clow, bstack, locvec, hout, hin, psend, precv, table, pick1, pick2,
    gsend, grecv, xsend, xrecv, zsend, zrecv, table2, osend, orecv, rsend, rrecv,
    load_sem, send_sem, recv_sem, xsem,
):
    y, k, z, x = (lax.axis_index(a) for a in AXES)
    r = y * NK + k
    c = z * NX + x

    def at_rx(r2, x2):
        return (lax.div(r2, NK), lax.rem(r2, NK), z, x2)

    def at_zx(z2, x2):
        return (y, k, z2, x2)

    def same_z_peer(p):
        peer = lax.rem(r * NX + x + p, NR * NX)
        return lax.div(peer, NX), lax.rem(peer, NX)

    def same_row_peer(p):
        peer = lax.rem(c + p, NZ * NX)
        return lax.div(peer, NX), lax.rem(peer, NX)

    def send(stage, src, dst, where, sem=None):
        pltpu.make_async_remote_copy(
            src_ref=src, dst_ref=dst, send_sem=send_sem.at[stage], recv_sem=recv_sem.at[stage] if sem is None else sem,
            device_id=where, device_id_type=MESH,
        ).start()

    def landed(ref, sem):
        pltpu.make_async_copy(ref, ref, sem).wait()

    loads = [
        pltpu.make_async_copy(basis_hbm, basis, load_sem.at[0]),
        pltpu.make_async_copy(cinv_hbm, cinv, load_sem.at[1]),
        pltpu.make_async_copy(linv_hbm, linv, load_sem.at[2]),
    ]
    barrier = pltpu.get_barrier_semaphore()

    @pl.loop(1, NR * NX)
    def _(p):
        r2, x2 = same_z_peer(p)
        pl.semaphore_signal(barrier, inc=1, device_id=at_rx(r2, x2), device_id_type=MESH)

    @pl.loop(0, (NZ - 1) * NX)
    def _(p):
        z2 = lax.rem(z + 1 + lax.div(p, NX), NZ)
        pl.semaphore_signal(barrier, inc=1, device_id=at_zx(z2, lax.rem(p, NX)), device_id_type=MESH)

    for load in loads:
        load.start()

    blocks = [resid[:, b * BLK:(b + 1) * BLK] for b in range(OWN // BLK)]
    for d in range(4):
        which = ib[0, d]
        block = blocks[0]
        for b in range(1, OWN // BLK):
            block = jnp.where(which == b, blocks[b], block)
        hout[d] = block
    locvec[:, :OWN] = resid[...]

    sub = lax.broadcasted_iota(jnp.int32, (LANES, LANES), 0)
    sub16 = lax.broadcasted_iota(jnp.int32, (16, LANES), 0)
    lane16 = lax.broadcasted_iota(jnp.int32, (16, LANES), 1).astype(F32)

    def invert(g, total):
        rows = slots[pl.ds(g * 8, 8), :]
        low = rows & (LANES - 1)
        high = lax.shift_right_logical(rows, 7) - z * 16
        picks, values = [], []
        for u in range(8):
            entry = g * 8 + u
            row = lax.rem(lax.div(entry, 2), NZ) * 16 + lax.div(entry, 16) * 2 + (u & 1)
            picks.append((low[u:u + 1] == sub).astype(F32).astype(BF16))
            here = high[u:u + 1] == sub16
            values.append(jnp.concatenate(
                [jnp.where(here, row.astype(F32), 0.0), jnp.where(here, lane16, 0.0)], axis=0).astype(BF16))
        return total + dot_nt(jnp.concatenate(picks, axis=1), jnp.concatenate(values, axis=1))

    inverse = lax.fori_loop(0, 16, invert, jnp.zeros((LANES, 32), F32)).T.astype(jnp.int32)
    from_row, from_lane = inverse[:16], inverse[16:]
    my_slots = slots[pl.ds(r * 16, 16), :]
    want_row, want_lane = lax.shift_right_logical(my_slots, 7), my_slots & (LANES - 1)
    for a in range(16):
        for pick, row in ((pick1, from_row), (pick2, want_row)):
            hot = (row[a:a + 1] == sub).astype(F32).astype(BF16)
            pick[:LANES, a * LANES:(a + 1) * LANES] = hot
            pick[LANES:, a * LANES:(a + 1) * LANES] = hot

    def gather(source, pick, lane):
        high, low = halves(source.T)
        stacked = jnp.concatenate([high, low], axis=1)
        rows = []
        for a in range(0, 16, 2):
            picked = dot(stacked, pick[:, a * LANES:(a + 2) * LANES])
            for h in range(2):
                mine = lane[a + h:a + h + 1] == sub
                rows.append(jnp.sum(jnp.where(mine, picked[:, h * LANES:(h + 1) * LANES], 0.0), axis=0, keepdims=True))
        return jnp.concatenate(rows, axis=0)

    loads[0].wait()
    bhigh, blow = halves(basis[...])
    bstack[0:NEV] = bhigh
    bstack[NEV:2 * NEV] = bhigh
    bstack[2 * NEV:3 * NEV] = blow

    pl.semaphore_wait(barrier, NR * NX - 1 + (NZ - 1) * NX)

    r_up, r_down = lax.rem(r + 1, NR), lax.rem(r + NR - 1, NR)
    c_up, c_down = lax.rem(c + 1, NZ * NX), lax.rem(c + NZ * NX - 1, NZ * NX)
    sides = (
        at_rx(r_up, x), at_rx(r_down, x),
        at_zx(lax.div(c_up, NX), lax.rem(c_up, NX)), at_zx(lax.div(c_down, NX), lax.rem(c_down, NX)),
    )
    inside = (r > 0, r < NR - 1, c > 0, c < NZ * NX - 1)
    inside_back = (r < NR - 1, r > 0, c < NZ * NX - 1, c > 0)
    for d in range(4):
        send(0, hout.at[d], hin.at[d], sides[d])

    loads[1].wait()

    def split(i, _):
        rows = pl.ds(i * 64, 64)
        high, low = halves(cinv[rows, :])
        chigh[rows, :] = high
        clow[rows, :] = low
        return 0

    lax.fori_loop(0, PART // 64, split, 0)

    landed(hin, recv_sem.at[0])
    for d in range(4):
        locvec[:, OWN + d * BLK:OWN + (d + 1) * BLK] = jnp.where(inside[d], hin[d], jnp.zeros_like(hin[d]))

    vec = locvec[...]
    low2 = jnp.concatenate([bstack[2 * NEV:], bstack[2 * NEV:]], axis=0)
    partial = dot_nt(vec, bstack[:2 * NEV]) + dot_nt(vec, low2)
    psend[...] = partial.reshape(RHS, 1, LANES)
    me = r * NX + x
    precv[pl.ds(me, 1)] = psend[pl.ds(me, 1)]

    @pl.loop(1, NR * NX)
    def _(p):
        r2, x2 = same_z_peer(p)
        send(1, psend.at[r2 * NX + x2], precv.at[me], at_rx(r2, x2))

    loads[2].wait()
    schwarz = dot_nt(vec, linv[...])
    landed(precv.at[pl.ds(0, NR * NX - 1)], recv_sem.at[1])

    got = precv[...].reshape(16, 2, LANES)
    first = lax.broadcasted_iota(jnp.int32, (16, LANES), 1) < NEV
    mine = pl.ds(pl.multiple_of(z * 16, 16), 16)
    table[mine, :] = jnp.where(first, got[:, 0], got[:, 1])

    @pl.loop(1, NZ)
    def _(p):
        send(2, table.at[mine], table.at[mine], at_zx(lax.rem(z + p, NZ), x))

    landed(table.at[pl.ds(0, (NZ - 1) * 16)], recv_sem.at[2])

    gsend[...] = gather(table[...], pick1, from_lane).reshape(NX, 4, LANES)
    grecv[pl.ds(me, 1)] = gsend[pl.ds(x, 1)]

    @pl.loop(1, NR * NX)
    def _(p):
        r2, x2 = same_z_peer(p)
        send(3, gsend.at[x2], grecv.at[me], at_rx(r2, x2))

    landed(grecv.at[pl.ds(0, NR * NX - 1)], recv_sem.at[3])

    rhigh, rlow = halves(jnp.concatenate([grecv[:, a, :] for a in range(4)], axis=1))
    both = jnp.concatenate([rhigh, rlow], axis=0)
    for n in range(CHUNKS):
        def product(i, _):
            cols = pl.ds(n * WIDTH + i * 256, 256)
            top = dot_nt(both, chigh[cols, :])
            part = top[:RHS] + top[RHS:] + dot_nt(rhigh, clow[cols, :])
            xsend[n, :, :, pl.ds(pl.multiple_of(i * 256, 256), 256)] = part.reshape(NX, NZ, 256)
            return 0

        lax.fori_loop(0, WIDTH // 256, product, 0)

        @pl.loop(1, NX)
        def _(p):
            x2 = lax.rem(x + p, NX)
            send(4, xsend.at[n, x2], xrecv.at[n, p - 1], at_zx(z, x2), xsem.at[n])

    for n in range(CHUNKS):
        landed(xrecv.at[n], xsem.at[n])
        total = xsend[n, pl.ds(x, 1)][0]
        for p in range(NX - 1):
            total = total + xrecv[n, p]
        for j in range(ROWS):
            zsend[n, :, j, :] = total[:, j * LANES:(j + 1) * LANES]

        @pl.loop(1, NZ)
        def _(p):
            z2 = lax.rem(z + p, NZ)
            send(5, zsend.at[n, z2], zrecv.at[p - 1, n], at_zx(z2, x))

    landed(zrecv, recv_sem.at[5])
    mine2 = pl.ds(pl.multiple_of(r * 16, 16), 16)
    total = zsend[:, pl.ds(z, 1)].reshape(16, LANES)
    for p in range(NZ - 1):
        total = total + zrecv[p].reshape(16, LANES)
    table2[mine2, :] = total

    @pl.loop(1, NR)
    def _(p):
        send(6, table2.at[mine2], table2.at[mine2], at_rx(lax.rem(r + p, NR), x))

    landed(table2.at[pl.ds(0, (NR - 1) * 16)], recv_sem.at[6])

    osend[...] = gather(table2[...], pick2, want_lane).reshape(16, 1, LANES)
    q = x * NZ + z
    orecv[pl.ds(q, 1)] = osend[pl.ds(lax.div(c, 2), 1)]

    @pl.loop(1, NZ * NX)
    def _(p):
        z2, x2 = same_row_peer(p)
        send(7, osend.at[z2 * 2 + lax.div(x2, 2)], orecv.at[q], at_zx(z2, x2))

    landed(orecv.at[pl.ds(0, NZ * NX - 1)], recv_sem.at[7])
    entries = orecv[...].reshape(RHS, LANES)
    high, low = halves(jnp.where(lax.rem(x, 2) == 1, entries[:, NEV:], entries[:, :NEV]))
    coarse = jnp.concatenate([high, low, high], axis=1)

    back = dot(coarse, bstack[:, OWN:])
    for d in range(4):
        rsend[d] = back[:, d * BLK:(d + 1) * BLK]
    opposite = (1, 0, 3, 2)
    for d in range(4):
        send(8, rsend.at[d], rrecv.at[d], sides[opposite[d]])
    result = schwarz + dot(coarse, bstack[:, :OWN])
    landed(rrecv, recv_sem.at[8])
    parts = [result[:, b * BLK:(b + 1) * BLK] for b in range(OWN // BLK)]
    for d in range(4):
        returned = jnp.where(inside_back[d], rrecv[d], jnp.zeros_like(rrecv[d]))
        which = ib[0, d]
        for b in range(OWN // BLK):
            parts[b] = parts[b] + jnp.where(which == b, returned, jnp.zeros_like(returned))
    for b in range(OWN // BLK):
        out[:, b * BLK:(b + 1) * BLK] = parts[b]

    for stage, ref in (
        (0, hout), (1, psend.at[pl.ds(0, NR * NX - 1)]), (2, table.at[pl.ds(0, (NZ - 1) * 16)]),
        (3, grecv.at[pl.ds(0, NR * NX - 1)]), (4, xrecv), (5, zrecv), (6, table2.at[pl.ds(0, (NR - 1) * 16)]),
        (7, orecv.at[pl.ds(0, NZ * NX - 1)]), (8, rsend),
    ):
        landed(ref, send_sem.at[stage])


def local(residuals, intersect_blocks, local_inverse, coarse_basis, coarse_slots, coarse_inverse):
    vmem = pl.BlockSpec(memory_space=pltpu.VMEM)
    hbm = pl.BlockSpec(memory_space=pl.ANY)
    result = pl.pallas_call(
        kernel,
        out_shape=jax.ShapeDtypeStruct((RHS, OWN), F32),
        in_specs=[pl.BlockSpec(memory_space=pltpu.SMEM), vmem, vmem, hbm, hbm, hbm],
        out_specs=vmem,
        scratch_shapes=[
            pltpu.VMEM((NEV, LOC), F32),
            pltpu.VMEM((OWN, LOC), BF16),
            pltpu.VMEM((PART, OWN), F32),
            pltpu.VMEM((PART, OWN), BF16),
            pltpu.VMEM((PART, OWN), BF16),
            pltpu.VMEM((3 * NEV, LOC), BF16),
            pltpu.VMEM((RHS, LOC), BF16),
            pltpu.VMEM((4, RHS, BLK), BF16),
            pltpu.VMEM((4, RHS, BLK), BF16),
            pltpu.VMEM((RHS, 1, LANES), F32),
            pltpu.VMEM((RHS, 1, LANES), F32),
            pltpu.VMEM((LANES, LANES), F32),
            pltpu.VMEM((2 * LANES, PART), BF16),
            pltpu.VMEM((2 * LANES, PART), BF16),
            pltpu.VMEM((NX, 4, LANES), F32),
            pltpu.VMEM((RHS, 4, LANES), F32),
            pltpu.VMEM((CHUNKS, NX, NZ, WIDTH), F32),
            pltpu.VMEM((CHUNKS, NX - 1, NZ, WIDTH), F32),
            pltpu.VMEM((CHUNKS, NZ, ROWS, LANES), F32),
            pltpu.VMEM((NZ - 1, CHUNKS, ROWS, LANES), F32),
            pltpu.VMEM((LANES, LANES), F32),
            pltpu.VMEM((16, 1, LANES), F32),
            pltpu.VMEM((RHS, 1, LANES), F32),
            pltpu.VMEM((4, RHS, BLK), F32),
            pltpu.VMEM((4, RHS, BLK), F32),
            pltpu.SemaphoreType.DMA((3,)),
            pltpu.SemaphoreType.DMA((9,)),
            pltpu.SemaphoreType.DMA((9,)),
            pltpu.SemaphoreType.DMA((CHUNKS,)),
        ],
        compiler_params=pltpu.CompilerParams(collective_id=0, has_side_effects=True),
        name="schwarz",
    )(
        intersect_blocks, residuals.T, coarse_slots.reshape(LANES, LANES), coarse_basis.T, local_inverse, coarse_inverse
    )
    return result.T


def solution(mesh):
    torus = Mesh(mesh.devices.reshape(NY, NK, NZ, NX), AXES)
    in_specs = (
        P(ROW_COL, None),
        P(ROW_COL, None),
        P(ROW_COL, None),
        P(ROW_COL, None),
        P(),
        P(ROW, COL),
    )
    return jax.shard_map(local, mesh=torus, in_specs=in_specs, out_specs=P(ROW_COL, None), check_vma=False)
```

```python
import functools

import jax
import jax.numpy as jnp
from jax import lax
from jax.experimental import pallas as pl
from jax.experimental.pallas import tpu as pltpu
from jax.sharding import Mesh
from jax.sharding import PartitionSpec as P

MESH = pl.DeviceIdType.MESH
AXES = ("row_0", "row_1", "col_0", "col_1")
ROW_COL = AXES
ROW = AXES[:2]
COL = AXES[2:]
NY, NK, NZ, NX = 4, 2, 8, 4
NR = NY * NK
BLK = 128
OWN = 512
LOC = 1024
NEV = 64
RHS = 32
LANES = 128
PART = 2048
CHUNKS = 4
WIDTH = PART // CHUNKS
ROWS = WIDTH // LANES
F32 = jnp.float32
BF16 = jnp.bfloat16
NT = (((1,), (1,)), ((), ()))


def away(d, n):
    return min(d, n - d)


FAR_YKX = sorted(
    ((dy, dk, dx) for dy in range(NY) for dk in range(NK) for dx in range(NX) if (dy, dk, dx) != (0, 0, 0)),
    key=lambda d: -away(d[0], NY) - away(d[2], NX))
FAR_ZX = sorted(
    ((dz, dx) for dz in range(NZ) for dx in range(NX) if (dz, dx) != (0, 0)), key=lambda d: -away(d[0], NZ) - away(d[1], NX))
FAR_YK = sorted(((dy, dk) for dy in range(NY) for dk in range(NK) if (dy, dk) != (0, 0)), key=lambda d: -away(d[0], NY))
FAR_Z = sorted(range(1, NZ), key=lambda d: -away(d, NZ))
FAR_X = sorted(range(1, NX), key=lambda d: -away(d, NX))


def dot(a, b):
    return jnp.dot(a, b, preferred_element_type=F32)


def dot_nt(a, b):
    return lax.dot_general(a, b, NT, preferred_element_type=F32)


def halves(x):
    high = x.astype(BF16)
    return high, (x - high.astype(F32)).astype(BF16)


def kernel(
    ib, resid_hbm, slots_hbm, basis_hbm, linv_hbm, cinv_hbm, out,
    resid, slots, basis, linv, cinv, chigh, clow, bstack, hout, hin, psend, precv, table, pick1, pick2,
    gsend, grecv, xsend, xrecv, zsend, zrecv, table2, osend, orecv, rsend, rrecv,
    load_sem, send_sem, recv_sem, xsem,
):
    y, k, z, x = (lax.axis_index(a) for a in AXES)
    r = y * NK + k
    c = z * NX + x
    ys = [lax.rem(y + d, NY) for d in range(NY)]
    ks = [lax.rem(k + d, NK) for d in range(NK)]
    zs = [lax.rem(z + d, NZ) for d in range(NZ)]
    xs = [lax.rem(x + d, NX) for d in range(NX)]

    def at_rx(r2, x2):
        return (lax.div(r2, NK), lax.rem(r2, NK), z, x2)

    def at_zx(z2, x2):
        return (y, k, z2, x2)

    def send(stage, src, dst, where, sem=None):
        pltpu.make_async_remote_copy(
            src_ref=src, dst_ref=dst, send_sem=send_sem.at[stage], recv_sem=recv_sem.at[stage] if sem is None else sem,
            device_id=where, device_id_type=MESH,
        ).start()

    def landed(ref, sem):
        pltpu.make_async_copy(ref, ref, sem).wait()

    loads = [
        pltpu.make_async_copy(resid_hbm, resid, load_sem.at[0]),
        pltpu.make_async_copy(basis_hbm, basis, load_sem.at[1]),
        pltpu.make_async_copy(slots_hbm, slots, load_sem.at[2]),
        pltpu.make_async_copy(linv_hbm, linv, load_sem.at[3]),
        pltpu.make_async_copy(cinv_hbm, cinv, load_sem.at[4]),
    ]
    loads[0].start()
    barrier = pltpu.get_barrier_semaphore()
    for dz, dx in FAR_ZX:
        if dz > 0:
            pl.semaphore_signal(barrier, inc=1, device_id=at_zx(zs[dz], xs[dx]), device_id_type=MESH)
    for dy, dk, dx in FAR_YKX:
        pl.semaphore_signal(barrier, inc=1, device_id=(ys[dy], ks[dk], z, xs[dx]), device_id_type=MESH)
    for load in loads[1:]:
        load.start()

    loads[0].wait()
    blocks = [resid[:, b * BLK:(b + 1) * BLK] for b in range(OWN // BLK)]
    for d in range(4):
        which = ib[0, d]
        block = blocks[0]
        for b in range(1, OWN // BLK):
            block = jnp.where(which == b, blocks[b], block)
        hout[d] = block

    loads[1].wait()
    bhigh, blow = halves(basis[...])
    for half in range(2):
        bstack[2 * half * NEV:(2 * half + 1) * NEV] = bhigh
        bstack[(2 * half + 1) * NEV:(2 * half + 2) * NEV] = blow

    pl.semaphore_wait(barrier, NR * NX - 1 + (NZ - 1) * NX)

    r_up, r_down = lax.rem(r + 1, NR), lax.rem(r + NR - 1, NR)
    c_up, c_down = lax.rem(c + 1, NZ * NX), lax.rem(c + NZ * NX - 1, NZ * NX)
    sides = (
        at_rx(r_up, x), at_rx(r_down, x),
        at_zx(lax.div(c_up, NX), lax.rem(c_up, NX)), at_zx(lax.div(c_down, NX), lax.rem(c_down, NX)),
    )
    inside = (r > 0, r < NR - 1, c > 0, c < NZ * NX - 1)
    inside_back = (r < NR - 1, r > 0, c < NZ * NX - 1, c > 0)
    for d in range(4):
        send(0, hout.at[d], hin.at[d], sides[d])

    own = dot_nt(resid[...], bstack[:2 * NEV, :OWN])
    sub = lax.broadcasted_iota(jnp.int32, (LANES, LANES), 0)
    loads[2].wait()
    my_slots = slots[pl.ds(r * 16, 16), :]
    want_row, want_lane = lax.shift_right_logical(my_slots, 7), my_slots & (LANES - 1)

    landed(hin, recv_sem.at[0])
    halo = jnp.concatenate([jnp.where(inside[d], hin[d], jnp.zeros_like(hin[d])) for d in range(4)], axis=1)

    split2 = own + dot_nt(halo, bstack[:2 * NEV, OWN:])
    psend[...] = (split2 + pltpu.roll(split2, NEV, 1)).reshape(RHS, 1, LANES)
    me = r * NX + x
    precv[pl.ds(me, 1)] = psend[pl.ds(me, 1)]
    group = [((ys[dy], ks[dk], z, xs[dx]), (ys[dy] * NK + ks[dk]) * NX + xs[dx], xs[dx]) for dy, dk, dx in FAR_YKX]
    for where, index, _ in group:
        send(1, psend.at[index], precv.at[me], where)

    sub16 = lax.broadcasted_iota(jnp.int32, (16, LANES), 0)
    lane16 = lax.broadcasted_iota(jnp.int32, (16, LANES), 1).astype(F32)

    def invert(g, total):
        rows = slots[pl.ds(g * 8, 8), :]
        low = rows & (LANES - 1)
        high = lax.shift_right_logical(rows, 7) - z * 16
        picks, values = [], []
        for u in range(8):
            entry = g * 8 + u
            row = lax.rem(lax.div(entry, 2), NZ) * 16 + lax.div(entry, 16) * 2 + (u & 1)
            picks.append((low[u:u + 1] == sub).astype(F32).astype(BF16))
            here = high[u:u + 1] == sub16
            values.append(jnp.concatenate(
                [jnp.where(here, row.astype(F32), 0.0), jnp.where(here, lane16, 0.0)], axis=0).astype(BF16))
        return total + dot_nt(jnp.concatenate(picks, axis=1), jnp.concatenate(values, axis=1))

    def one_hot(pick, row):
        for a in range(16):
            hot = (row[a:a + 1] == sub).astype(F32).astype(BF16)
            pick[:LANES, a * LANES:(a + 1) * LANES] = hot
            pick[LANES:, a * LANES:(a + 1) * LANES] = hot

    inverse = lax.fori_loop(0, 16, invert, jnp.zeros((LANES, 32), F32)).T.astype(jnp.int32)
    from_row, from_lane = inverse[:16], inverse[16:]
    one_hot(pick1, from_row)

    def gather(source, pick, lane):
        high, low = halves(source.T)
        stacked = jnp.concatenate([high, low], axis=1)
        rows = []
        for a in range(0, 16, 2):
            picked = dot(stacked, pick[:, a * LANES:(a + 2) * LANES])
            for h in range(2):
                mine = lane[a + h:a + h + 1] == sub
                rows.append(jnp.sum(jnp.where(mine, picked[:, h * LANES:(h + 1) * LANES], 0.0), axis=0, keepdims=True))
        return jnp.concatenate(rows, axis=0)

    landed(precv.at[pl.ds(0, NR * NX - 1)], recv_sem.at[1])

    got = precv[...].reshape(16, 2, LANES)
    first = lax.broadcasted_iota(jnp.int32, (16, LANES), 1) < NEV
    mine = pl.ds(pl.multiple_of(z * 16, 16), 16)
    table[mine, :] = jnp.where(first, got[:, 0], got[:, 1])
    for dz in FAR_Z:
        send(2, table.at[mine], table.at[mine], at_zx(zs[dz], x))

    loads[3].wait()
    schwarz = dot_nt(resid[...], linv[:, :OWN]) + dot_nt(halo, linv[:, OWN:])
    loads[4].wait()

    def split(i, _):
        rows = pl.ds(i * 64, 64)
        high, low = halves(cinv[rows, :])
        chigh[rows, :] = high
        clow[rows, :] = low
        return 0

    lax.fori_loop(0, PART // 128, split, 0)

    landed(table.at[pl.ds(0, (NZ - 1) * 16)], recv_sem.at[2])

    gsend[...] = gather(table[...], pick1, from_lane).reshape(NX, 4, LANES)
    grecv[pl.ds(me, 1)] = gsend[pl.ds(x, 1)]
    for where, _, x2 in group:
        send(3, gsend.at[x2], grecv.at[me], where)

    lax.fori_loop(PART // 128, PART // 64, split, 0)

    landed(grecv.at[pl.ds(0, NR * NX - 1)], recv_sem.at[3])

    rhigh, rlow = halves(jnp.concatenate([grecv[:, a, :] for a in range(4)], axis=1))
    both = jnp.concatenate([rhigh, rlow], axis=0)
    for n in range(CHUNKS):
        for i in range(WIDTH // 256):
            rows = pl.ds(n * WIDTH + i * 256, 256)
            top = dot_nt(both, chigh[rows, :])
            part = top[:RHS] + top[RHS:] + dot_nt(rhigh, clow[rows, :])
            xsend[n, :, :, i * 256:(i + 1) * 256] = part.reshape(NX, NZ, 256)
        for dx in FAR_X:
            send(4, xsend.at[n, xs[dx]], xrecv.at[n, dx - 1], at_zx(z, xs[dx]), xsem.at[n])

    one_hot(pick2, want_row)

    for n in range(CHUNKS):
        landed(xrecv.at[n], xsem.at[n])
        total = xsend[n, pl.ds(x, 1)][0]
        for p in range(NX - 1):
            total = total + xrecv[n, p]
        for j in range(ROWS):
            zsend[n, :, j, :] = total[:, j * LANES:(j + 1) * LANES]
        for dz in FAR_Z:
            send(5, zsend.at[n, zs[dz]], zrecv.at[dz - 1, n], at_zx(zs[dz], x))

    landed(zrecv, recv_sem.at[5])
    mine2 = pl.ds(pl.multiple_of(r * 16, 16), 16)
    total = zsend[:, pl.ds(z, 1)].reshape(16, LANES)
    for p in range(NZ - 1):
        total = total + zrecv[p].reshape(16, LANES)
    table2[mine2, :] = total

    for dy, dk in FAR_YK:
        send(6, table2.at[mine2], table2.at[mine2], (ys[dy], ks[dk], z, x))

    landed(table2.at[pl.ds(0, (NR - 1) * 16)], recv_sem.at[6])

    osend[...] = gather(table2[...], pick2, want_lane).reshape(16, 1, LANES)
    q = x * NZ + z
    orecv[pl.ds(q, 1)] = osend[pl.ds(lax.div(c, 2), 1)]
    for dz, dx in FAR_ZX:
        send(7, osend.at[zs[dz] * 2 + lax.div(xs[dx], 2)], orecv.at[q], at_zx(zs[dz], xs[dx]))

    landed(orecv.at[pl.ds(0, NZ * NX - 1)], recv_sem.at[7])
    entries = orecv[...].reshape(RHS, LANES)
    high, low = halves(jnp.where(lax.rem(x, 2) == 1, entries[:, NEV:], entries[:, :NEV]))
    coarse = jnp.concatenate([high, high, low, low], axis=1)

    back = dot(coarse, bstack[:, OWN:])
    for d in range(4):
        rsend[d] = back[:, d * BLK:(d + 1) * BLK]
    opposite = (1, 0, 3, 2)
    for d in range(4):
        send(8, rsend.at[d], rrecv.at[d], sides[opposite[d]])
    result = schwarz + dot(coarse, bstack[:, :OWN])
    landed(rrecv, recv_sem.at[8])
    parts = [result[:, b * BLK:(b + 1) * BLK] for b in range(OWN // BLK)]
    for d in range(4):
        returned = jnp.where(inside_back[d], rrecv[d], jnp.zeros_like(rrecv[d]))
        which = ib[0, d]
        for b in range(OWN // BLK):
            parts[b] = parts[b] + jnp.where(which == b, returned, jnp.zeros_like(returned))
    for b in range(OWN // BLK):
        out[:, b * BLK:(b + 1) * BLK] = parts[b]

    for stage, ref in (
        (0, hout), (1, psend.at[pl.ds(0, NR * NX - 1)]), (2, table.at[pl.ds(0, (NZ - 1) * 16)]),
        (3, grecv.at[pl.ds(0, NR * NX - 1)]), (4, xrecv), (5, zrecv), (6, table2.at[pl.ds(0, (NR - 1) * 16)]),
        (7, orecv.at[pl.ds(0, NZ * NX - 1)]), (8, rsend),
    ):
        landed(ref, send_sem.at[stage])


def local(residuals, intersect_blocks, local_inverse, coarse_basis, coarse_slots, coarse_inverse):
    vmem = pl.BlockSpec(memory_space=pltpu.VMEM)
    hbm = pl.BlockSpec(memory_space=pl.ANY)
    arrays = (
        intersect_blocks, residuals.T, coarse_slots.reshape(LANES, LANES), coarse_basis.T, local_inverse, coarse_inverse
    )
    result = pl.pallas_call(
        kernel,
        out_shape=jax.ShapeDtypeStruct((RHS, OWN), F32),
        in_specs=[pl.BlockSpec(memory_space=pltpu.SMEM)] + [hbm] * 5,
        out_specs=vmem,
        scratch_shapes=[
            pltpu.VMEM((RHS, OWN), BF16),
            pltpu.VMEM((LANES, LANES), jnp.int32),
            pltpu.VMEM((NEV, LOC), F32),
            pltpu.VMEM((OWN, LOC), BF16),
            pltpu.VMEM((PART, OWN), F32),
            pltpu.VMEM((PART, OWN), BF16),
            pltpu.VMEM((PART, OWN), BF16),
            pltpu.VMEM((4 * NEV, LOC), BF16),
            pltpu.VMEM((4, RHS, BLK), BF16),
            pltpu.VMEM((4, RHS, BLK), BF16),
            pltpu.VMEM((RHS, 1, LANES), F32),
            pltpu.VMEM((RHS, 1, LANES), F32),
            pltpu.VMEM((LANES, LANES), F32),
            pltpu.VMEM((2 * LANES, PART), BF16),
            pltpu.VMEM((2 * LANES, PART), BF16),
            pltpu.VMEM((NX, 4, LANES), F32),
            pltpu.VMEM((RHS, 4, LANES), F32),
            pltpu.VMEM((CHUNKS, NX, NZ, WIDTH), F32),
            pltpu.VMEM((CHUNKS, NX - 1, NZ, WIDTH), F32),
            pltpu.VMEM((CHUNKS, NZ, ROWS, LANES), F32),
            pltpu.VMEM((NZ - 1, CHUNKS, ROWS, LANES), F32),
            pltpu.VMEM((LANES, LANES), F32),
            pltpu.VMEM((16, 1, LANES), F32),
            pltpu.VMEM((RHS, 1, LANES), F32),
            pltpu.VMEM((4, RHS, BLK), F32),
            pltpu.VMEM((4, RHS, BLK), F32),
            pltpu.SemaphoreType.DMA((5,)),
            pltpu.SemaphoreType.DMA((9,)),
            pltpu.SemaphoreType.DMA((9,)),
            pltpu.SemaphoreType.DMA((CHUNKS,)),
        ],
        compiler_params=pltpu.CompilerParams(collective_id=0, has_side_effects=True, vmem_limit_bytes=32 * 2**20),
        name="schwarz",
    )(*(pltpu.with_memory_space_constraint(array, pltpu.HBM) for array in arrays))
    return result.T


def solution(mesh):
    torus = Mesh(mesh.devices.reshape(NY, NK, NZ, NX), AXES)
    in_specs = (
        P(ROW_COL, None),
        P(ROW_COL, None),
        P(ROW_COL, None),
        P(ROW_COL, None),
        P(),
        P(ROW, COL),
    )
    return jax.shard_map(local, mesh=torus, in_specs=in_specs, out_specs=P(ROW_COL, None), check_vma=False)
```

```python
import functools

import jax
import jax.numpy as jnp
from jax import lax
from jax.experimental import pallas as pl
from jax.experimental.pallas import tpu as pltpu
from jax.sharding import Mesh
from jax.sharding import PartitionSpec as P

MESH = pl.DeviceIdType.MESH
AXES = ("row_0", "row_1", "col_0", "col_1")
ROW_COL = AXES
ROW = AXES[:2]
COL = AXES[2:]
NY, NK, NZ, NX = 4, 2, 8, 4
NR = NY * NK
BLK = 128
OWN = 512
LOC = 1024
NEV = 64
RHS = 32
LANES = 128
PART = 2048
CHUNKS = 4
WIDTH = PART // CHUNKS
ROWS = WIDTH // LANES
F32 = jnp.float32
BF16 = jnp.bfloat16
NT = (((1,), (1,)), ((), ()))


def away(d, n):
    return min(d, n - d)


FAR_YKX = sorted(
    ((dy, dk, dx) for dy in range(NY) for dk in range(NK) for dx in range(NX) if (dy, dk, dx) != (0, 0, 0)),
    key=lambda d: -away(d[0], NY) - away(d[2], NX))
FAR_ZX = sorted(
    ((dz, dx) for dz in range(NZ) for dx in range(NX) if (dz, dx) != (0, 0)), key=lambda d: -away(d[0], NZ) - away(d[1], NX))
FAR_YK = sorted(((dy, dk) for dy in range(NY) for dk in range(NK) if (dy, dk) != (0, 0)), key=lambda d: -away(d[0], NY))
FAR_Z = sorted(range(1, NZ), key=lambda d: -away(d, NZ))
FAR_X = sorted(range(1, NX), key=lambda d: -away(d, NX))


def dot(a, b):
    return jnp.dot(a, b, preferred_element_type=F32)


def dot_nt(a, b):
    return lax.dot_general(a, b, NT, preferred_element_type=F32)


def halves(x):
    high = x.astype(BF16)
    return high, (x - high.astype(F32)).astype(BF16)


def kernel(
    ib_hbm, resid_hbm, slots_hbm, basis_hbm, linv_hbm, cinv_hbm, out,
    ib, resid, slots, basis, linv, cinv, chigh, clow, bstack, hout, hin, psend, precv, table, pick1, pick2,
    gsend, grecv, xsend, xrecv, zsend, zrecv, table2, osend, orecv, nrecv, nbasis,
    load_sem, send_sem, recv_sem, xsem,
):
    y, k, z, x = (lax.axis_index(a) for a in AXES)
    r = y * NK + k
    c = z * NX + x
    ys = [lax.rem(y + d, NY) for d in range(NY)]
    ks = [lax.rem(k + d, NK) for d in range(NK)]
    zs = [lax.rem(z + d, NZ) for d in range(NZ)]
    xs = [lax.rem(x + d, NX) for d in range(NX)]

    def at_rx(r2, x2):
        return (lax.div(r2, NK), lax.rem(r2, NK), z, x2)

    def at_zx(z2, x2):
        return (y, k, z2, x2)

    def send(stage, src, dst, where, sem=None):
        pltpu.make_async_remote_copy(
            src_ref=src, dst_ref=dst, send_sem=send_sem.at[stage], recv_sem=recv_sem.at[stage] if sem is None else sem,
            device_id=where, device_id_type=MESH,
        ).start()

    def landed(ref, sem):
        pltpu.make_async_copy(ref, ref, sem).wait()

    loads = [
        pltpu.make_async_copy(resid_hbm, resid, load_sem.at[0]),
        pltpu.make_async_copy(basis_hbm, basis, load_sem.at[1]),
        pltpu.make_async_copy(slots_hbm, slots, load_sem.at[2]),
        pltpu.make_async_copy(linv_hbm, linv, load_sem.at[3]),
        pltpu.make_async_copy(cinv_hbm, cinv, load_sem.at[4]),
        pltpu.make_async_copy(ib_hbm, ib, load_sem.at[5]),
    ]
    loads[0].start()
    loads[5].start()
    barrier = pltpu.get_barrier_semaphore()
    for dz in FAR_Z:
        pl.semaphore_signal(barrier, inc=1, device_id=at_zx(zs[dz], x), device_id_type=MESH)
    for dy, dk, dx in FAR_YKX:
        pl.semaphore_signal(barrier, inc=1, device_id=(ys[dy], ks[dk], z, xs[dx]), device_id_type=MESH)

    @pl.when(x == NX - 1)
    def _():
        pl.semaphore_signal(barrier, inc=1, device_id=at_zx(zs[1], 0), device_id_type=MESH)

    @pl.when(x == 0)
    def _():
        pl.semaphore_signal(barrier, inc=1, device_id=at_zx(zs[NZ - 1], NX - 1), device_id_type=MESH)

    for load in loads[1:5]:
        load.start()

    loads[0].wait()
    loads[5].wait()
    blocks = [resid[:, b * BLK:(b + 1) * BLK] for b in range(OWN // BLK)]
    for d in range(4):
        which = ib[0, d]
        block = blocks[0]
        for b in range(1, OWN // BLK):
            block = jnp.where(which == b, blocks[b], block)
        hout[d] = block

    loads[1].wait()
    bhigh, blow = halves(basis[...])
    bstack[:NEV] = bhigh
    bstack[NEV:] = blow
    osend[0] = jnp.zeros((1, LANES), F32)
    osend[17] = jnp.zeros((1, LANES), F32)

    pl.semaphore_wait(barrier, NR * NX - 1 + NZ - 1 + jnp.where(x == NX - 1, 1, 0) + jnp.where(x == 0, 1, 0))

    r_up, r_down = lax.rem(r + 1, NR), lax.rem(r + NR - 1, NR)
    c_up, c_down = lax.rem(c + 1, NZ * NX), lax.rem(c + NZ * NX - 1, NZ * NX)
    sides = (
        at_rx(r_up, x), at_rx(r_down, x),
        at_zx(lax.div(c_up, NX), lax.rem(c_up, NX)), at_zx(lax.div(c_down, NX), lax.rem(c_down, NX)),
    )
    inside = (r > 0, r < NR - 1, c > 0, c < NZ * NX - 1)
    inside_back = (r < NR - 1, r > 0, c < NZ * NX - 1, c > 0)
    for d in range(4):
        send(0, hout.at[d], hin.at[d], sides[d])

    own = dot_nt(resid[...], bstack[:, :OWN])
    sub = lax.broadcasted_iota(jnp.int32, (LANES, LANES), 0)
    loads[2].wait()
    my_slots = slots[pl.ds(r * 16, 16), :]
    want_row, want_lane = lax.shift_right_logical(my_slots, 7), my_slots & (LANES - 1)

    landed(hin, recv_sem.at[0])
    halo = jnp.concatenate([jnp.where(inside[d], hin[d], jnp.zeros_like(hin[d])) for d in range(4)], axis=1)

    split2 = own + dot_nt(halo, bstack[:, OWN:])
    psend[...] = (split2 + pltpu.roll(split2, NEV, 1)).reshape(RHS, 1, LANES)
    me = r * NX + x
    precv[pl.ds(me, 1)] = psend[pl.ds(me, 1)]
    group = [((ys[dy], ks[dk], z, xs[dx]), (ys[dy] * NK + ks[dk]) * NX + xs[dx], xs[dx]) for dy, dk, dx in FAR_YKX]
    for where, index, _ in group:
        send(1, psend.at[index], precv.at[me], where)

    for d in range(4):
        send(8, bstack.at[:, pl.ds(OWN + d * BLK, BLK)], nbasis.at[d], sides[(1, 0, 3, 2)[d]])

    sub16 = lax.broadcasted_iota(jnp.int32, (16, LANES), 0)
    lane16 = lax.broadcasted_iota(jnp.int32, (16, LANES), 1).astype(F32)

    def invert(g, total):
        rows = slots[pl.ds(g * 8, 8), :]
        low = rows & (LANES - 1)
        high = lax.shift_right_logical(rows, 7) - z * 16
        picks, values = [], []
        for u in range(8):
            entry = g * 8 + u
            row = lax.rem(lax.div(entry, 2), NZ) * 16 + lax.div(entry, 16) * 2 + (u & 1)
            picks.append((low[u:u + 1] == sub).astype(F32).astype(BF16))
            here = high[u:u + 1] == sub16
            values.append(jnp.concatenate(
                [jnp.where(here, row.astype(F32), 0.0), jnp.where(here, lane16, 0.0)], axis=0).astype(BF16))
        return total + dot_nt(jnp.concatenate(picks, axis=1), jnp.concatenate(values, axis=1))

    def one_hot(pick, row):
        for a in range(16):
            hot = (row[a:a + 1] == sub).astype(F32).astype(BF16)
            pick[:LANES, a * LANES:(a + 1) * LANES] = hot
            pick[LANES:, a * LANES:(a + 1) * LANES] = hot

    inverse = lax.fori_loop(0, 16, invert, jnp.zeros((LANES, 32), F32)).T.astype(jnp.int32)
    from_row, from_lane = inverse[:16], inverse[16:]
    one_hot(pick1, from_row)

    def gather(source, pick, lane):
        high, low = halves(source.T)
        stacked = jnp.concatenate([high, low], axis=1)
        rows = []
        for a in range(0, 16, 2):
            picked = dot(stacked, pick[:, a * LANES:(a + 2) * LANES])
            for h in range(2):
                mine = lane[a + h:a + h + 1] == sub
                rows.append(jnp.sum(jnp.where(mine, picked[:, h * LANES:(h + 1) * LANES], 0.0), axis=0, keepdims=True))
        return jnp.concatenate(rows, axis=0)

    landed(precv.at[pl.ds(0, NR * NX - 1)], recv_sem.at[1])

    got = precv[...].reshape(16, 2, LANES)
    first = lax.broadcasted_iota(jnp.int32, (16, LANES), 1) < NEV
    mine = pl.ds(pl.multiple_of(z * 16, 16), 16)
    table[mine, :] = jnp.where(first, got[:, 0], got[:, 1])
    for dz in FAR_Z:
        send(2, table.at[mine], table.at[mine], at_zx(zs[dz], x))

    loads[3].wait()
    schwarz = dot_nt(resid[...], linv[:, :OWN]) + dot_nt(halo, linv[:, OWN:])
    loads[4].wait()

    def split(i, _):
        rows = pl.ds(i * 64, 64)
        high, low = halves(cinv[rows, :])
        chigh[rows, :] = high
        clow[rows, :] = low
        return 0

    lax.fori_loop(0, PART // 128, split, 0)

    landed(table.at[pl.ds(0, (NZ - 1) * 16)], recv_sem.at[2])

    gsend[...] = gather(table[...], pick1, from_lane).reshape(NX, 4, LANES)
    grecv[pl.ds(me, 1)] = gsend[pl.ds(x, 1)]
    for where, _, x2 in group:
        send(3, gsend.at[x2], grecv.at[me], where)

    lax.fori_loop(PART // 128, PART // 64, split, 0)

    landed(grecv.at[pl.ds(0, NR * NX - 1)], recv_sem.at[3])

    rhigh, rlow = halves(jnp.concatenate([grecv[:, a, :] for a in range(4)], axis=1))
    both = jnp.concatenate([rhigh, rlow], axis=0)
    for n in range(CHUNKS):
        for i in range(WIDTH // 256):
            rows = pl.ds(n * WIDTH + i * 256, 256)
            top = dot_nt(both, chigh[rows, :])
            part = top[:RHS] + top[RHS:] + dot_nt(rhigh, clow[rows, :])
            xsend[n, :, :, i * 256:(i + 1) * 256] = part.reshape(NX, NZ, 256)
        for dx in FAR_X:
            send(4, xsend.at[n, xs[dx]], xrecv.at[n, dx - 1], at_zx(z, xs[dx]), xsem.at[n])

    one_hot(pick2, want_row)

    for n in range(CHUNKS):
        landed(xrecv.at[n], xsem.at[n])
        total = xsend[n, pl.ds(x, 1)][0]
        for p in range(NX - 1):
            total = total + xrecv[n, p]
        for j in range(ROWS):
            zsend[n, :, j, :] = total[:, j * LANES:(j + 1) * LANES]
        for dz in FAR_Z:
            send(5, zsend.at[n, zs[dz]], zrecv.at[dz - 1, n], at_zx(zs[dz], x))

    landed(zrecv, recv_sem.at[5])
    mine2 = pl.ds(pl.multiple_of(r * 16, 16), 16)
    total = zsend[:, pl.ds(z, 1)].reshape(16, LANES)
    for p in range(NZ - 1):
        total = total + zrecv[p].reshape(16, LANES)
    table2[mine2, :] = total

    for dy, dk in FAR_YK:
        send(6, table2.at[mine2], table2.at[mine2], (ys[dy], ks[dk], z, x))

    landed(table2.at[pl.ds(0, (NR - 1) * 16)], recv_sem.at[6])

    osend[1:17] = gather(table2[...], pick2, want_lane).reshape(16, 1, LANES)
    q = x * NZ + z
    orecv[pl.ds(q, 1)] = osend[pl.ds(z * 2 + lax.div(x + 1, 2), 2)].reshape(1, 2, 1, LANES)
    y_up, k_up = lax.div(r_up, NK), lax.rem(r_up, NK)
    y_down, k_down = lax.div(r_down, NK), lax.rem(r_down, NK)
    for dz, dx in FAR_ZX + [(0, 0)]:
        pair = osend.at[zs[dz] * 2 + lax.div(xs[dx], 2) + 1]
        send(9, pair, nrecv.at[0, q], (y_down, k_down, zs[dz], xs[dx]))
        send(9, pair, nrecv.at[1, q], (y_up, k_up, zs[dz], xs[dx]))
        if (dz, dx) != (0, 0):
            send(7, osend.at[pl.ds(zs[dz] * 2 + lax.div(xs[dx] + 1, 2), 2)], orecv.at[q], at_zx(zs[dz], xs[dx]))

    landed(nbasis, recv_sem.at[8])
    landed(orecv.at[pl.ds(0, NZ * NX - 1)], recv_sem.at[7])
    landed(nrecv, recv_sem.at[9])

    def prolonged(entries, vectors):
        high, low = halves(entries)
        stacked = jnp.concatenate([jnp.concatenate([part, part], axis=1) for part in (high, low)], axis=0)
        both = dot(stacked, vectors)
        return both[:RHS] + both[RHS:]

    odd = lax.rem(x, 2) == 1
    pairs = jnp.concatenate([orecv[:, h].reshape(RHS, LANES) for h in range(2)], axis=1)
    line = jnp.where(odd, pairs[:, :3 * NEV], pairs[:, NEV:])
    beside = [nrecv[h].reshape(RHS, LANES) for h in range(2)]
    sources = [jnp.where(odd, pair[:, NEV:], pair[:, :NEV]) for pair in beside] + [line[:, 2 * NEV:], line[:, :NEV]]
    result = schwarz + prolonged(line[:, NEV:2 * NEV], bstack[:, :OWN])
    parts = [result[:, b * BLK:(b + 1) * BLK] for b in range(OWN // BLK)]
    for d in range(4):
        returned = prolonged(sources[d], nbasis[d])
        returned = jnp.where(inside_back[d], returned, jnp.zeros_like(returned))
        which = ib[0, d]
        for b in range(OWN // BLK):
            parts[b] = parts[b] + jnp.where(which == b, returned, jnp.zeros_like(returned))
    for b in range(OWN // BLK):
        out[:, b * BLK:(b + 1) * BLK] = parts[b]

    for stage, ref in (
        (0, hout), (1, psend.at[pl.ds(0, NR * NX - 1)]), (2, table.at[pl.ds(0, (NZ - 1) * 16)]),
        (3, grecv.at[pl.ds(0, NR * NX - 1)]), (4, xrecv), (5, zrecv), (6, table2.at[pl.ds(0, (NR - 1) * 16)]),
        (7, orecv.at[pl.ds(0, NZ * NX - 1)]), (8, nbasis), (9, nrecv),
    ):
        landed(ref, send_sem.at[stage])


def local(residuals, intersect_blocks, local_inverse, coarse_basis, coarse_slots, coarse_inverse):
    vmem = pl.BlockSpec(memory_space=pltpu.VMEM)
    hbm = pl.BlockSpec(memory_space=pl.ANY)
    arrays = (
        intersect_blocks, residuals.T, coarse_slots.reshape(LANES, LANES), coarse_basis.T, local_inverse, coarse_inverse
    )
    result = pl.pallas_call(
        kernel,
        out_shape=jax.ShapeDtypeStruct((RHS, OWN), F32),
        in_specs=[hbm] * 6,
        out_specs=vmem,
        scratch_shapes=[
            pltpu.SMEM((1, 4), jnp.int32),
            pltpu.VMEM((RHS, OWN), BF16),
            pltpu.VMEM((LANES, LANES), jnp.int32),
            pltpu.VMEM((NEV, LOC), F32),
            pltpu.VMEM((OWN, LOC), BF16),
            pltpu.VMEM((PART, OWN), F32),
            pltpu.VMEM((PART, OWN), BF16),
            pltpu.VMEM((PART, OWN), BF16),
            pltpu.VMEM((2 * NEV, LOC), BF16),
            pltpu.VMEM((4, RHS, BLK), BF16),
            pltpu.VMEM((4, RHS, BLK), BF16),
            pltpu.VMEM((RHS, 1, LANES), F32),
            pltpu.VMEM((RHS, 1, LANES), F32),
            pltpu.VMEM((LANES, LANES), F32),
            pltpu.VMEM((2 * LANES, PART), BF16),
            pltpu.VMEM((2 * LANES, PART), BF16),
            pltpu.VMEM((NX, 4, LANES), F32),
            pltpu.VMEM((RHS, 4, LANES), F32),
            pltpu.VMEM((CHUNKS, NX, NZ, WIDTH), F32),
            pltpu.VMEM((CHUNKS, NX - 1, NZ, WIDTH), F32),
            pltpu.VMEM((CHUNKS, NZ, ROWS, LANES), F32),
            pltpu.VMEM((NZ - 1, CHUNKS, ROWS, LANES), F32),
            pltpu.VMEM((LANES, LANES), F32),
            pltpu.VMEM((18, 1, LANES), F32),
            pltpu.VMEM((RHS, 2, 1, LANES), F32),
            pltpu.VMEM((2, RHS, 1, LANES), F32),
            pltpu.VMEM((4, 2 * NEV, BLK), BF16),
            pltpu.SemaphoreType.DMA((6,)),
            pltpu.SemaphoreType.DMA((10,)),
            pltpu.SemaphoreType.DMA((10,)),
            pltpu.SemaphoreType.DMA((CHUNKS,)),
        ],
        compiler_params=pltpu.CompilerParams(collective_id=0, has_side_effects=True, vmem_limit_bytes=32 * 2**20),
        name="schwarz",
    )(*(pltpu.with_memory_space_constraint(array, pltpu.HBM) for array in arrays))
    return result.T


def solution(mesh):
    torus = Mesh(mesh.devices.reshape(NY, NK, NZ, NX), AXES)
    in_specs = (
        P(ROW_COL, None),
        P(ROW_COL, None),
        P(ROW_COL, None),
        P(ROW_COL, None),
        P(),
        P(ROW, COL),
    )
    return jax.shard_map(local, mesh=torus, in_specs=in_specs, out_specs=P(ROW_COL, None), check_vma=False)
```
